32 devices in a mesh: groups: 2 (over x), strip: 16 (over z, y, core).
Axes of the slice: x: 2, y: 2, z: 4, core: 2. Of those that a mesh axis runs over, the one named last changes fastest.
Arguments:
- incoming_wave: float32 [8, 2, 256, 1024], P('groups', None, 'strip'), parts along dimension 0, may hold values from -64 to 64
- speed_class_map: int32 [4, 256, 1024], P('groups', 'strip'), parts along dimension 0, may hold values from 0 to 15
- spectral_entry_index: int32 [8, 4], P('groups'), parts along dimension 0, may hold values from 0 to 15
- filter_weights: float32 [16, 16, 2, 13], replicated, may hold values from -1.6 to 1.6
- scaled_pulsations: float32 [16], replicated, may hold values from 1 to 6
- inverse_speed_classes: float32 [16], replicated, may hold values from 0.3 to 1.5
Outputs:
- image: float32 [4, 256, 1024], P('groups', 'strip'), parts along dimension 0
- handed: float32 [8, 2, 256, 1024], P('groups', None, 'strip'), parts along dimension 0
The draws below stay inside these ranges and needn't reach their ends.
There are 2 independent parts, one for each index of `groups`. The reference program is written for one: setup_inputs(seed, part) draws one part's arguments, and reference() takes and returns one part's arrays. A program takes and returns all parts, laid end to end along the dimension named above; an argument that names none is the same for every part. Nothing has to cross between parts.
All inputs are finite; a program needn't handle non-finite values.
Results may differ from the reference program's by a relative error of at most 0.0003.
Values sent between devices are 32-bit elements; how exact they have to be, the bound alone decides.
A program may use at most 128 MiB of HBM per device.

```python
import math
import jax
import jax.numpy as jnp
from jax import lax

NY = 1024
SECTIONS = 4
LEVELS = 2
ORDER = 12
NFREQ = 4
NBIN = 16
NW = 16
SIDEWAYS_COUNT = 64


def draw_incoming_wave(key, part):
    noise_key = jax.random.fold_in(jax.random.fold_in(key, 11), 0)
    total_rows = SECTIONS * SIDEWAYS_COUNT
    shifted_rows = (jnp.arange(total_rows, dtype=jnp.int32) - SIDEWAYS_COUNT // 2) % total_rows
    position = (shifted_rows % SIDEWAYS_COUNT).astype(jnp.float32) / max(SIDEWAYS_COUNT - 1, 1)
    profile = jnp.exp(jnp.log(3.0) * position)[None, None, :, None]
    base = jnp.clip(jax.random.normal(noise_key, (NFREQ, 2, total_rows, NY), jnp.float32), -6.0, 6.0)
    return base * profile


def touch_ends(values, rng, smallest, top_value):
    longest = values.shape.index(max(values.shape))
    spots = []
    for shift in (0, 1):
        where = [jax.random.randint(jax.random.fold_in(rng, axis), (), 0, length) for axis, length in enumerate(values.shape)]
        where[longest] = (where[longest] + shift) % values.shape[longest]
        spots.append(tuple(where))
    return values.at[spots[0]].set(smallest).at[spots[1]].set(top_value)


def scatter_about(own_key, dims, spread, bound, kind=jnp.bfloat16):
    drawn = spread * jax.random.normal(own_key, dims, jnp.float32)
    return jnp.clip(drawn, min=-bound, max=bound).astype(kind)


def setup_inputs(seed: int = 0, part: int = 0) -> dict:
    streams_of = jax.random.split(jax.random.key(seed), 7)
    part_splits = jax.random.split(jax.random.fold_in(streams_of[6], part), 7)
    return {
        "incoming_wave": draw_incoming_wave(jax.random.fold_in(jax.random.fold_in(streams_of[6], part), 71), part),
        "speed_class_map": touch_ends(jax.random.randint(part_splits[1], (LEVELS, SECTIONS * SIDEWAYS_COUNT, NY), 0, NBIN), jax.random.fold_in(part_splits[1], 1), 0, NBIN - 1).astype(jnp.int32),
        "spectral_entry_index": touch_ends(jax.random.randint(part_splits[2], (SECTIONS, NFREQ), 0, NW), jax.random.fold_in(part_splits[2], 1), 0, NW - 1).astype(jnp.int32),
        "filter_weights": scatter_about(streams_of[3], (NW, NBIN, 2, ORDER + 1), 0.28, 1.6, jnp.float32),
        "scaled_pulsations": jnp.clip(jnp.exp(jax.random.uniform(streams_of[4], (NW,), jnp.float32, math.log(1.0), math.log(6.0))), 1.0, 6.0),
        "inverse_speed_classes": jnp.clip(jnp.exp(jax.random.uniform(streams_of[5], (NBIN,), jnp.float32, math.log(0.3), math.log(1.5))), 0.3, 1.5),
    }


def stencil_padded(padded):
    vertical = padded[:, :, :-2, :] + padded[:, :, 2:, :]
    middle = padded[:, :, 1:-1, :]
    return -0.5 * middle[..., 1:-1] + 0.25 * (vertical[..., 1:-1] + middle[..., :-2] + middle[..., 2:]) + 0.125 * (vertical[..., :-2] + vertical[..., 2:])

def mcclellan_step(field):
    return stencil_padded(jnp.pad(field, ((0, 0), (0, 0), (1, 1), (1, 1))))

def complex_times(coeff, field):
    real_part = coeff[:, 0] * field[:, 0] - coeff[:, 1] * field[:, 1]
    imag_part = coeff[:, 0] * field[:, 1] + coeff[:, 1] * field[:, 0]
    return jnp.stack([real_part, imag_part], axis=1)

def image_downward(field, speed_strata, freq_row, filter_weights, scaled_pulsations, inverse_speed_classes):
    highest = lax.Precision.HIGHEST
    freq_select = (freq_row[:, None] == jnp.arange(NW, dtype=jnp.int32)[None, :]).astype(jnp.float32)
    freq_coeffs = jnp.einsum('fw,wbck->fbck', freq_select, filter_weights, precision=highest)
    freq_omega = jnp.dot(freq_select, scaled_pulsations, precision=highest)
    wavefield = field
    raws = []
    for level in range(LEVELS):
        cells = speed_strata[level].reshape(-1)
        bin_onehot = (cells[None, :] == jnp.arange(NBIN, dtype=jnp.int32)[:, None]).astype(jnp.float32)
        cell_slowness = jnp.dot(inverse_speed_classes, bin_onehot, precision=highest).reshape(SIDEWAYS_COUNT, NY)
        table = jnp.einsum('fbck,bn->kfcn', freq_coeffs, bin_onehot, precision=highest).reshape(ORDER + 1, NFREQ, 2, SIDEWAYS_COUNT, NY)
        previous = wavefield
        current = mcclellan_step(wavefield)
        accumulated = complex_times(table[0], previous) + complex_times(table[1], current)
        for order_index in range(2, ORDER + 1):
            following = 2.0 * mcclellan_step(current) - previous
            accumulated = accumulated + complex_times(table[order_index], following)
            previous, current = (current, following)
        phase_angle = freq_omega[:, None, None] * cell_slowness[None]
        cosine = jnp.cos(phase_angle)
        sine_part = jnp.sin(phase_angle)
        real_part = accumulated[:, 0] * cosine - accumulated[:, 1] * sine_part
        imag_part = accumulated[:, 0] * sine_part + accumulated[:, 1] * cosine
        wavefield = jnp.stack([real_part, imag_part], axis=1)
        raws.append(lax.optimization_barrier(jnp.sum(real_part, axis=0)))
    return (wavefield, raws)

def reference(incoming_wave, speed_class_map, spectral_entry_index, filter_weights, scaled_pulsations, inverse_speed_classes):
    half_shift = SIDEWAYS_COUNT // 2
    incoming_wave = jnp.roll(incoming_wave, -half_shift, axis=2)
    speed_class_map = jnp.roll(speed_class_map, -half_shift, axis=1)
    bottoms = []
    images = []
    handed_parts = []
    for vertical_slab in range(SECTIONS):
        speed_strata = speed_class_map[:, vertical_slab * SIDEWAYS_COUNT:(vertical_slab + 1) * SIDEWAYS_COUNT, :]
        above_floor_lines, above_unscaled_waves = image_downward(incoming_wave[:, :, vertical_slab * SIDEWAYS_COUNT:(vertical_slab + 1) * SIDEWAYS_COUNT, :], speed_strata, spectral_entry_index[vertical_slab], filter_weights, scaled_pulsations, inverse_speed_classes)
        bottoms.append(above_floor_lines)
        if vertical_slab == 0:
            totals = above_unscaled_waves
            handed_parts.append(above_floor_lines)
        else:
            second_bottom, second_raws = image_downward(bottoms[vertical_slab - 1], speed_strata, spectral_entry_index[vertical_slab - 1], filter_weights, scaled_pulsations, inverse_speed_classes)
            totals = [above_unscaled_waves[level] + second_raws[level] for level in range(LEVELS)]
            handed_parts.append(second_bottom)
        section_images = []
        for level in range(LEVELS):
            raw_image = totals[level]
            mean_square = jnp.sum(raw_image * raw_image) / (SIDEWAYS_COUNT * NY)
            section_images.append(raw_image / jnp.sqrt(mean_square + 1e-06))
        images.append(jnp.stack(section_images, axis=0))
    image = jnp.roll(jnp.concatenate(images, axis=1), half_shift, axis=1)
    handed = jnp.roll(jnp.concatenate(handed_parts, axis=2), half_shift, axis=2)
    return (image, handed)
```

```python
import functools
import jax
import jax.numpy as jnp
from jax import lax
from jax.experimental import pallas as pl
from jax.experimental.pallas import tpu as pltpu
from jax.sharding import PartitionSpec as P

SECTIONS = 4
LEVELS = 2
ORDER = 12
NFREQ = 4
NBIN = 16
NW = 16


def extended_2(shard, sides, width):
    for axis, dim in sides:
        devices, length = (lax.axis_size(axis), shard.shape[dim])
        up = [(i, (i + 1) % devices) for i in range(devices)]
        down = [(j, i) for i, j in up]
        last = lax.slice_in_dim(shard, length - width, length, axis=dim)
        initial = lax.slice_in_dim(shard, 0, width, axis=dim)
        before = lax.ppermute(last, axis, up)
        after = lax.ppermute(initial, axis, down)
        shard = jnp.concatenate([before, shard, after], axis=dim)
    return shard


def from_behind(shard, axis, by):
    devices = lax.axis_size(axis)
    return lax.ppermute(shard, axis, [(i, (i + by) % devices) for i in range(devices)])


def stencil_padded(padded):
    vertical = padded[:, :, :-2, :] + padded[:, :, 2:, :]
    middle = padded[:, :, 1:-1, :]
    return (
        -0.5 * middle[..., 1:-1]
        + 0.25 * (vertical[..., 1:-1] + middle[..., :-2] + middle[..., 2:])
        + 0.125 * (vertical[..., :-2] + vertical[..., 2:])
    )


def complex_times(coeff, field):
    real_part = coeff[:, 0] * field[:, 0] - coeff[:, 1] * field[:, 1]
    imag_part = coeff[:, 0] * field[:, 1] + coeff[:, 1] * field[:, 0]
    return jnp.stack([real_part, imag_part], axis=1)


def shards(
    incoming_wave,
    speed_class_map,
    spectral_entry_index,
    filter_weights,
    scaled_pulsations,
    inverse_speed_classes,
):
    highest = lax.Precision.HIGHEST
    summed_along = incoming_wave.shape[2]
    summed_across = incoming_wave.shape[3]
    strip_count = lax.axis_size("strip")
    lateral_count = strip_count // SECTIONS
    position = (lax.axis_index("strip") - lateral_count // 2) % strip_count
    vertical_slab = position // lateral_count
    lateral_place = position % lateral_count
    section_rows = summed_along * lateral_count
    section_cells = section_rows * summed_across
    margin = ORDER
    extended_rows = summed_along + 2 * margin
    lateral_rows = (
        lateral_place * summed_along - margin + jnp.arange(extended_rows, dtype=jnp.int32)
    )
    inside = ((lateral_rows >= 0) & (lateral_rows < section_rows)).astype(jnp.float32)[
        None, None, :, None
    ]

    def mcclellan_step(field):
        padded = jnp.pad(field, ((0, 0), (0, 0), (1, 1), (0, 0)))
        padded = jnp.pad(padded, ((0, 0), (0, 0), (0, 0), (1, 1)))
        result = stencil_padded(padded)
        result = result * inside
        return result

    def interior(field):
        return field[:, :, margin : margin + summed_along, :]

    def image_downward(field, batch_index):
        freq_row = lax.dynamic_index_in_dim(spectral_entry_index, batch_index, 0, keepdims=False)
        freq_select = (freq_row[:, None] == jnp.arange(NW, dtype=jnp.int32)[None, :]).astype(
            jnp.float32
        )
        freq_coeffs = jnp.einsum("fw,wbck->fbck", freq_select, filter_weights, precision=highest)
        freq_omega = jnp.dot(freq_select, scaled_pulsations, precision=highest)
        wavefield = field
        raws = []
        for level in range(LEVELS):
            cells = speed_class_map[level].reshape(-1)
            bin_onehot = (cells[None, :] == jnp.arange(NBIN, dtype=jnp.int32)[:, None]).astype(
                jnp.float32
            )
            cell_slowness = jnp.dot(inverse_speed_classes, bin_onehot, precision=highest).reshape(
                summed_along, summed_across
            )
            table = jnp.einsum("fbck,bn->kfcn", freq_coeffs, bin_onehot, precision=highest).reshape(
                ORDER + 1, NFREQ, 2, summed_along, summed_across
            )
            extended = extended_2(wavefield, (("strip", 2),), ORDER) * inside
            previous = extended
            current = mcclellan_step(extended)
            accumulated = complex_times(table[0], interior(previous)) + complex_times(
                table[1], interior(current)
            )

            def recursion_step(order_index, state_tuple):
                before, present, running = state_tuple
                following = 2.0 * mcclellan_step(present) - before
                coeff = lax.dynamic_index_in_dim(table, order_index, 0, keepdims=False)
                running = running + complex_times(coeff, interior(following))
                return (present, following, running)

            previous, current, accumulated = lax.fori_loop(
                2, ORDER + 1, recursion_step, (previous, current, accumulated)
            )
            phase_angle = freq_omega[:, None, None] * cell_slowness[None]
            cosine = jnp.cos(phase_angle)
            sine_part = jnp.sin(phase_angle)
            real_part = accumulated[:, 0] * cosine - accumulated[:, 1] * sine_part
            imag_part = accumulated[:, 0] * sine_part + accumulated[:, 1] * cosine
            wavefield = jnp.stack([real_part, imag_part], axis=1)
            raws.append(jnp.sum(real_part, axis=0))
        return (wavefield, raws)

    above_floor_lines, above_unscaled_waves = image_downward(incoming_wave, vertical_slab)
    arriving = from_behind(above_floor_lines, "strip", lateral_count)
    second_bottom, second_raws = image_downward(arriving, jnp.maximum(vertical_slab - 1, 0))
    handed = jnp.where(vertical_slab == 0, above_floor_lines, second_bottom)
    first_section = (vertical_slab > 0).astype(jnp.float32)
    totals = [
        above_unscaled_waves[level] + first_section * second_raws[level] for level in range(LEVELS)
    ]
    selector = (jnp.arange(SECTIONS, dtype=jnp.int32) == vertical_slab).astype(jnp.float32)
    images = []
    for level in range(LEVELS):
        raw_image = totals[level]
        spread = lax.psum(selector * jnp.sum(raw_image * raw_image), "strip")
        mean_square = jnp.sum(spread * selector) / section_cells
        images.append(raw_image / jnp.sqrt(mean_square + 1e-06))
    return (jnp.stack(images, axis=0), handed)


SUB = 8
LANES = 128
PAD = 1
UNROLL = 4
MESH = pl.DeviceIdType.MESH


def at_row(row):
    return pl.ds(pl.multiple_of(row * SUB, SUB), SUB)


def kernel(
    strip_count,
    entry_ref,
    wave_ref,
    map_ref,
    table_ref,
    image_ref,
    handed_ref,
    starts,
    work,
    bottom,
    last,
    last_in,
    wave_out,
    map_out,
    map_all,
    raw,
    raw_in,
    sum_own,
    sum_in,
    swap_sems,
    halo_sems,
    hand_sems,
    fin_sems,
    raw_sems,
    sum_sems,
):
    nfh = wave_ref.shape[0] // 2
    length = wave_ref.shape[2]
    rows = 2 * length
    blocks = wave_ref.shape[3] // LANES
    lateral = strip_count // SECTIONS
    shift = lateral // 2
    pairs = lateral // 2
    margin = ORDER
    first = PAD + margin
    me = lax.axis_index("strip")
    position = lax.rem(me + strip_count - shift, strip_count)
    section = position // lateral
    place = lax.rem(position, lateral)
    pair = place // 2
    half = lax.rem(place, 2)
    up = jnp.where(pair > 0, 1, 0)
    down = jnp.where(pair < pairs - 1, 1, 0)
    has_up = pair > 0
    has_down = pair < pairs - 1
    has_before = section > 0
    has_after = section < SECTIONS - 1
    other = 1 - half

    def device(pos):
        return {"strip": lax.rem(pos + shift + strip_count, strip_count)}

    partner = device(position + 1 - 2 * half)
    upper = device(position - 2)
    lower = device(position + 2)
    deeper = device(position + lateral)
    shallower = device(position + strip_count - lateral)

    def remote(src, dst, sems, index, target):
        return pltpu.make_async_remote_copy(
            src_ref=src,
            dst_ref=dst,
            send_sem=sems.at[(0,) + index],
            recv_sem=sems.at[(1,) + index],
            device_id=target,
            device_id_type=MESH,
        )

    def span(row, count):
        return pl.ds(pl.multiple_of(row * SUB, SUB), count * SUB)

    zero = jnp.zeros((SUB, LANES), jnp.float32)
    for edge in (first - 1, first + rows):
        for f in range(nfh):
            for c in range(2):
                for s in range(2 * LEVELS):
                    starts[s, f, c, at_row(edge), :] = zero
        for c in range(2):
            for k in range(ORDER):
                work[k, c, at_row(edge), :] = zero

    barrier = pltpu.get_barrier_semaphore()
    for d in range(1, lateral):
        mate = device(section * lateral + lax.rem(place + d, lateral))
        pl.semaphore_signal(barrier, inc=1, device_id=mate, device_id_type=MESH)
    for target in (deeper, shallower):
        pl.semaphore_signal(barrier, inc=1, device_id=target, device_id_type=MESH)

    def rearrange(load, store):
        for g in range(length // SUB):
            for j in range(blocks):
                store(g, j, load(g, j))

    def strided(row, g, j):
        return pl.ds((row + g * SUB) * SUB + j, SUB, stride=SUB)

    own_row = half * length
    for f in range(nfh):
        for c in range(2):
            rearrange(
                lambda g, j: wave_ref[other * nfh + f, c, pl.ds(g * SUB, SUB), pl.ds(j * LANES, LANES)],
                lambda g, j, x: pltpu_store(wave_out.at[f, c], strided(0, g, j), x),
            )
    for l in range(LEVELS):
        rearrange(
            lambda g, j: map_ref[l, pl.ds(g * SUB, SUB), pl.ds(j * LANES, LANES)],
            lambda g, j, x: pltpu_store(map_out.at[l], strided(0, g, j), x),
        )
    pl.semaphore_wait(barrier, lateral + 1)
    swaps = []
    for f in range(nfh):
        copy = remote(
            wave_out.at[f],
            starts.at[0, f, :, span(first + own_row, length), :],
            swap_sems,
            (f,),
            partner,
        )
        copy.start()
        swaps.append(copy)
    copy = remote(
        map_out, map_all.at[:, span(own_row, length), :], swap_sems, (nfh,), partner
    )
    copy.start()
    swaps.append(copy)
    for f in range(nfh):
        for c in range(2):
            rearrange(
                lambda g, j: wave_ref[half * nfh + f, c, pl.ds(g * SUB, SUB), pl.ds(j * LANES, LANES)],
                lambda g, j, x: pltpu_store(
                    starts.at[0, f, c], strided(first + own_row, g, j), x
                ),
            )
    for l in range(LEVELS):
        rearrange(
            lambda g, j: map_ref[l, pl.ds(g * SUB, SUB), pl.ds(j * LANES, LANES)],
            lambda g, j, x: pltpu_store(map_all.at[l], strided(own_row, g, j), x),
        )

    def halo_up(stage, f):
        ref = starts.at[stage, f]
        return remote(
            ref.at[:, span(first, margin), :],
            ref.at[:, span(first + rows, margin), :],
            halo_sems,
            (stage, f, 0),
            upper,
        )

    def halo_down(stage, f):
        ref = starts.at[stage, f]
        return remote(
            ref.at[:, span(first + rows - margin, margin), :],
            ref.at[:, span(first - margin, margin), :],
            halo_sems,
            (stage, f, 1),
            lower,
        )

    def send_halo(stage, f):
        pl.when(has_up)(lambda: halo_up(stage, f).start())
        pl.when(has_down)(lambda: halo_down(stage, f).start())

    def wait_halo(stage, f):
        pl.when(has_down)(lambda: halo_up(stage, f).wait_recv())
        pl.when(has_up)(lambda: halo_down(stage, f).wait_recv())

    def hand_parts(f):
        parts = ((0, margin), (rows - margin, margin), (margin, rows - 2 * margin))
        return [
            remote(
                bottom.at[f, :, span(row, count), :],
                starts.at[LEVELS, f, :, span(first + row, count), :],
                hand_sems,
                (f, n),
                deeper,
            )
            for n, (row, count) in enumerate(parts)
        ]

    lane = lax.broadcasted_iota(jnp.int32, (SUB, LANES), 1)
    sub = lax.broadcasted_iota(jnp.int32, (SUB, LANES), 0)
    at_first = lane == 0
    at_last = lane == LANES - 1
    keep_first = sub > 0
    keep_last = sub < SUB - 1

    def across(u):
        right = pltpu.roll(u, 1, 1)
        right_fix = jnp.where(keep_first, pltpu.roll(right, 1, 0), 0.0)
        left = pltpu.roll(u, LANES - 1, 1)
        left_fix = jnp.where(keep_last, pltpu.roll(left, SUB - 1, 0), 0.0)
        return jnp.where(at_first, right_fix, right) + jnp.where(at_last, left_fix, left)

    def reach(k):
        return ((margin - k + UNROLL - 1) // UNROLL) * UNROLL

    def apply(k, present, before, target):
        extra = reach(k)
        low = first - up * extra
        count = (rows + (up + down) * extra) // UNROLL

        def block(i, carry):
            base = low + i * UNROLL
            for c in range(2):
                v = [present[c, at_row(base - 1 + n), :] for n in range(UNROLL + 2)]
                q = [v[n] + v[n + 1] for n in range(UNROLL + 1)]
                for n in range(UNROLL):
                    u = q[n] + q[n + 1]
                    w = across(u) + (u + u)
                    centre = v[n + 1]
                    if before is None:
                        value = 0.125 * w - centre
                    else:
                        old = before[c, at_row(base + n), :]
                        value = 0.25 * w - (centre + centre + old)
                    target[c, at_row(base + n), :] = value
            return carry

        lax.fori_loop(0, count, block, 0)

    def unit(tick, level, f):
        stage = tick * LEVELS + level
        start = starts.at[stage, f]
        apply(1, start, None, work.at[0])
        apply(2, work.at[0], start, work.at[1])

        def step(k, carry):
            apply(k, work.at[k - 2], work.at[k - 3], work.at[k - 1])
            return carry

        lax.fori_loop(3, ORDER + 1, step, 0)
        batch = section if tick == 0 else jnp.maximum(section - 1, 0)
        entry = entry_ref[batch, half * nfh + f]

        def combine(i, carry):
            spots = [2 * i, 2 * i + 1]
            bins = [map_all[level, at_row(r), :] for r in spots]
            real = [None] * 2
            imag = [None] * 2
            for k in range(ORDER + 1):
                rows_of = [
                    jnp.broadcast_to(table_ref[entry, pl.ds(2 * k + c, 1), :], (SUB, LANES))
                    for c in range(2)
                ]
                source = start if k == 0 else work.at[k - 1]
                for n, r in enumerate(spots):
                    cr, ci = (
                        jnp.take_along_axis(t, bins[n], axis=1, mode="promise_in_bounds")
                        for t in rows_of
                    )
                    tr = source[0, at_row(first + r), :]
                    ti = source[1, at_row(first + r), :]
                    re = cr * tr - ci * ti
                    im = cr * ti + ci * tr
                    real[n] = re if k == 0 else real[n] + re
                    imag[n] = im if k == 0 else imag[n] + im
            for n, r in enumerate(spots):
                re, im = real[n], imag[n]
                if tick == 0 and f == 0:
                    raw[level, at_row(r), :] = re
                else:
                    part = re if tick == 0 else jnp.where(has_before, re, 0.0)
                    raw[level, at_row(r), :] = raw[level, at_row(r), :] + part
                for c, value in enumerate((re, im)):
                    if level < LEVELS - 1:
                        starts[stage + 1, f, c, at_row(first + r), :] = value
                    elif tick == 0:
                        bottom[f, c, at_row(r), :] = value
                    else:
                        last[f, c, at_row(r), :] = jnp.where(
                            has_before, value, bottom[f, c, at_row(r), :]
                        )
            return carry

        lax.fori_loop(0, rows // 2, combine, 0)

    def finish_wave(f):
        return remote(
            last.at[f, :, span(other * length, length), :],
            last_in.at[f],
            fin_sems,
            (f,),
            partner,
        )

    def finish_raw(l):
        return remote(
            raw.at[l, span(other * length, length), :], raw_in.at[l], raw_sems, (l,), partner
        )

    for f in range(nfh):
        swaps[f].wait_recv()
        send_halo(0, f)
    swaps[nfh].wait_recv()
    for level in range(LEVELS):
        for f in range(nfh):
            wait_halo(level, f)
            unit(0, level, f)
            if level < LEVELS - 1:
                send_halo(level + 1, f)
            else:

                @pl.when(has_after)
                def _():
                    for copy in hand_parts(f):
                        copy.start()

    def forward(f):
        @pl.when(has_before)
        def _():
            for copy in hand_parts(f):
                copy.wait_recv()

            send_halo(LEVELS, f)

    def skip_or(fn):
        pl.when(has_before)(fn)

    for f in range(nfh):
        forward(f)
    for level in range(LEVELS):
        for f in range(nfh):

            @pl.when(has_before)
            def _():
                wait_halo(LEVELS + level, f)

            unit(1, level, f)
            if level < LEVELS - 1:

                @pl.when(has_before)
                def _():
                    send_halo(LEVELS + level + 1, f)

            else:
                finish_wave(f).start()
        finish_raw(level).start()

    for l in range(LEVELS):
        finish_raw(l).wait_recv()

        def merge(i, carry):
            value = raw[l, at_row(own_row + i), :] + raw_in[l, at_row(i), :]
            raw_in[l, at_row(i), :] = value
            return carry + value * value

        sum_own[pl.ds(l * SUB, SUB), :] = lax.fori_loop(0, length, merge, zero)
    for d in range(1, lateral):
        mate = device(section * lateral + lax.rem(place + d, lateral))
        remote(sum_own, sum_in.at[d], sum_sems, (d,), mate).start()

    for f in range(nfh):
        for c in range(2):
            rearrange(
                lambda g, j: last[f, c, strided(own_row, g, j), :],
                lambda g, j, x: out_store(handed_ref, half * nfh + f, c, g, j, x),
            )
    for f in range(nfh):
        finish_wave(f).wait_recv()
        for c in range(2):
            rearrange(
                lambda g, j: last_in[f, c, strided(0, g, j), :],
                lambda g, j, x: out_store(handed_ref, other * nfh + f, c, g, j, x),
            )

    total = sum_own[...]
    for d in range(1, lateral):
        mate = device(section * lateral + lax.rem(place + d, lateral))
        remote(sum_own, sum_in.at[d], sum_sems, (d,), mate).wait_recv()
        total = total + sum_in[d]
    cells = length * lateral * blocks * LANES
    for l in range(LEVELS):
        mean = jnp.sum(total[l * SUB : (l + 1) * SUB], axis=(0, 1), keepdims=True) / cells
        scale = jnp.broadcast_to(1.0 / jnp.sqrt(mean + 1e-06), (SUB, LANES))

        def put(g, j, x):
            image_ref[l, pl.ds(g * SUB, SUB), pl.ds(j * LANES, LANES)] = x * scale

        rearrange(lambda g, j: raw_in[l, strided(0, g, j), :], put)

    for copy in swaps:
        copy.wait_send()
    for f in range(nfh):
        send_done = lambda make, stage: make(stage, f).wait_send()
        for stage in range(2 * LEVELS):
            live_up = has_up if stage < LEVELS else has_up & has_before
            live_down = has_down if stage < LEVELS else has_down & has_before
            pl.when(live_up)(lambda: send_done(halo_up, stage))
            pl.when(live_down)(lambda: send_done(halo_down, stage))

        @pl.when(has_after)
        def _():
            for copy in hand_parts(f):
                copy.wait_send()

        finish_wave(f).wait_send()
    for l in range(LEVELS):
        finish_raw(l).wait_send()
    for d in range(1, lateral):
        mate = device(section * lateral + lax.rem(place + d, lateral))
        remote(sum_own, sum_in.at[d], sum_sems, (d,), mate).wait_send()


def pltpu_store(ref, where, x):
    ref[where, :] = x


def out_store(ref, f, c, g, j, x):
    ref[f, c, pl.ds(g * SUB, SUB), pl.ds(j * LANES, LANES)] = x


def paired(
    incoming_wave,
    speed_class_map,
    spectral_entry_index,
    filter_weights,
    scaled_pulsations,
    inverse_speed_classes,
):
    strip_count = lax.axis_size("strip")
    lateral = strip_count // SECTIONS
    length = incoming_wave.shape[2]
    nfh = NFREQ // 2
    rows = 2 * length
    tall = (rows + 2 * ORDER + 2 * PAD) * SUB
    angle = scaled_pulsations[:, None] * inverse_speed_classes[None, :]
    cosine = jnp.cos(angle)[:, None, :]
    sine = jnp.sin(angle)[:, None, :]
    by_order = jnp.transpose(filter_weights, (2, 0, 3, 1))
    real = by_order[0] * cosine - by_order[1] * sine
    imag = by_order[0] * sine + by_order[1] * cosine
    table = jnp.stack([real, imag], axis=2).reshape(NW, 2 * (ORDER + 1), NBIN)
    table = jnp.pad(table, ((0, 0), (0, 0), (0, LANES - NBIN)))
    f32 = jnp.float32
    vmem = pl.BlockSpec(memory_space=pltpu.VMEM)

    def dma(*shape):
        return pltpu.SemaphoreType.DMA((2,) + shape)

    return pl.pallas_call(
        functools.partial(kernel, strip_count),
        out_shape=(
            jax.ShapeDtypeStruct(speed_class_map.shape, f32),
            jax.ShapeDtypeStruct(incoming_wave.shape, f32),
        ),
        in_specs=[pl.BlockSpec(memory_space=pltpu.SMEM), vmem, vmem, vmem],
        out_specs=(vmem, vmem),
        scratch_shapes=[
            pltpu.VMEM((2 * LEVELS, nfh, 2, tall, LANES), f32),
            pltpu.VMEM((ORDER, 2, tall, LANES), f32),
            pltpu.VMEM((nfh, 2, rows * SUB, LANES), f32),
            pltpu.VMEM((nfh, 2, rows * SUB, LANES), f32),
            pltpu.VMEM((nfh, 2, length * SUB, LANES), f32),
            pltpu.VMEM((nfh, 2, length * SUB, LANES), f32),
            pltpu.VMEM((LEVELS, length * SUB, LANES), jnp.int32),
            pltpu.VMEM((LEVELS, rows * SUB, LANES), jnp.int32),
            pltpu.VMEM((LEVELS, rows * SUB, LANES), f32),
            pltpu.VMEM((LEVELS, length * SUB, LANES), f32),
            pltpu.VMEM((LEVELS * SUB, LANES), f32),
            pltpu.VMEM((lateral, LEVELS * SUB, LANES), f32),
            dma(nfh + 1),
            dma(2 * LEVELS, nfh, 2),
            dma(nfh, 3),
            dma(nfh),
            dma(LEVELS),
            dma(lateral),
        ],
        compiler_params=pltpu.CompilerParams(
            collective_id=0, has_side_effects=True, vmem_limit_bytes=48 * 1024 * 1024
        ),
    )(spectral_entry_index, incoming_wave, speed_class_map, table)


def fits(mesh):
    lateral = mesh.shape["strip"] // SECTIONS
    return NFREQ % 2 == 0 and lateral % 4 == 0


def body_for(mesh):
    def body(wave, *rest):
        whole = wave.shape[3] == SUB * LANES and wave.shape[2] % SUB == 0
        if fits(mesh) and whole and wave.shape[2] >= ORDER:
            return paired(wave, *rest)
        return shards(wave, *rest)

    return body


def solution(mesh):
    return jax.shard_map(
        body_for(mesh),
        mesh=mesh,
        in_specs=(
            P("groups", None, "strip", None),
            P("groups", "strip", None),
            P("groups", None),
            P(),
            P(),
            P(),
        ),
        out_specs=(P("groups", "strip", None), P("groups", None, "strip", None)),
        check_vma=False,
    )
```

```python
import functools
import jax
import jax.numpy as jnp
from jax import lax
from jax.experimental import pallas as pl
from jax.experimental.pallas import tpu as pltpu
from jax.sharding import PartitionSpec as P

SECTIONS = 4
LEVELS = 2
ORDER = 12
NFREQ = 4
NBIN = 16
NW = 16


def extended_2(shard, sides, width):
    for axis, dim in sides:
        devices, length = (lax.axis_size(axis), shard.shape[dim])
        up = [(i, (i + 1) % devices) for i in range(devices)]
        down = [(j, i) for i, j in up]
        last = lax.slice_in_dim(shard, length - width, length, axis=dim)
        initial = lax.slice_in_dim(shard, 0, width, axis=dim)
        before = lax.ppermute(last, axis, up)
        after = lax.ppermute(initial, axis, down)
        shard = jnp.concatenate([before, shard, after], axis=dim)
    return shard


def from_behind(shard, axis, by):
    devices = lax.axis_size(axis)
    return lax.ppermute(shard, axis, [(i, (i + by) % devices) for i in range(devices)])


def stencil_padded(padded):
    vertical = padded[:, :, :-2, :] + padded[:, :, 2:, :]
    middle = padded[:, :, 1:-1, :]
    return (
        -0.5 * middle[..., 1:-1]
        + 0.25 * (vertical[..., 1:-1] + middle[..., :-2] + middle[..., 2:])
        + 0.125 * (vertical[..., :-2] + vertical[..., 2:])
    )


def complex_times(coeff, field):
    real_part = coeff[:, 0] * field[:, 0] - coeff[:, 1] * field[:, 1]
    imag_part = coeff[:, 0] * field[:, 1] + coeff[:, 1] * field[:, 0]
    return jnp.stack([real_part, imag_part], axis=1)


def shards(
    incoming_wave,
    speed_class_map,
    spectral_entry_index,
    filter_weights,
    scaled_pulsations,
    inverse_speed_classes,
):
    highest = lax.Precision.HIGHEST
    summed_along = incoming_wave.shape[2]
    summed_across = incoming_wave.shape[3]
    strip_count = lax.axis_size("strip")
    lateral_count = strip_count // SECTIONS
    position = (lax.axis_index("strip") - lateral_count // 2) % strip_count
    vertical_slab = position // lateral_count
    lateral_place = position % lateral_count
    section_rows = summed_along * lateral_count
    section_cells = section_rows * summed_across
    margin = ORDER
    extended_rows = summed_along + 2 * margin
    lateral_rows = (
        lateral_place * summed_along - margin + jnp.arange(extended_rows, dtype=jnp.int32)
    )
    inside = ((lateral_rows >= 0) & (lateral_rows < section_rows)).astype(jnp.float32)[
        None, None, :, None
    ]

    def mcclellan_step(field):
        padded = jnp.pad(field, ((0, 0), (0, 0), (1, 1), (0, 0)))
        padded = jnp.pad(padded, ((0, 0), (0, 0), (0, 0), (1, 1)))
        result = stencil_padded(padded)
        result = result * inside
        return result

    def interior(field):
        return field[:, :, margin : margin + summed_along, :]

    def image_downward(field, batch_index):
        freq_row = lax.dynamic_index_in_dim(spectral_entry_index, batch_index, 0, keepdims=False)
        freq_select = (freq_row[:, None] == jnp.arange(NW, dtype=jnp.int32)[None, :]).astype(
            jnp.float32
        )
        freq_coeffs = jnp.einsum("fw,wbck->fbck", freq_select, filter_weights, precision=highest)
        freq_omega = jnp.dot(freq_select, scaled_pulsations, precision=highest)
        wavefield = field
        raws = []
        for level in range(LEVELS):
            cells = speed_class_map[level].reshape(-1)
            bin_onehot = (cells[None, :] == jnp.arange(NBIN, dtype=jnp.int32)[:, None]).astype(
                jnp.float32
            )
            cell_slowness = jnp.dot(inverse_speed_classes, bin_onehot, precision=highest).reshape(
                summed_along, summed_across
            )
            table = jnp.einsum("fbck,bn->kfcn", freq_coeffs, bin_onehot, precision=highest).reshape(
                ORDER + 1, NFREQ, 2, summed_along, summed_across
            )
            extended = extended_2(wavefield, (("strip", 2),), ORDER) * inside
            previous = extended
            current = mcclellan_step(extended)
            accumulated = complex_times(table[0], interior(previous)) + complex_times(
                table[1], interior(current)
            )

            def recursion_step(order_index, state_tuple):
                before, present, running = state_tuple
                following = 2.0 * mcclellan_step(present) - before
                coeff = lax.dynamic_index_in_dim(table, order_index, 0, keepdims=False)
                running = running + complex_times(coeff, interior(following))
                return (present, following, running)

            previous, current, accumulated = lax.fori_loop(
                2, ORDER + 1, recursion_step, (previous, current, accumulated)
            )
            phase_angle = freq_omega[:, None, None] * cell_slowness[None]
            cosine = jnp.cos(phase_angle)
            sine_part = jnp.sin(phase_angle)
            real_part = accumulated[:, 0] * cosine - accumulated[:, 1] * sine_part
            imag_part = accumulated[:, 0] * sine_part + accumulated[:, 1] * cosine
            wavefield = jnp.stack([real_part, imag_part], axis=1)
            raws.append(jnp.sum(real_part, axis=0))
        return (wavefield, raws)

    above_floor_lines, above_unscaled_waves = image_downward(incoming_wave, vertical_slab)
    arriving = from_behind(above_floor_lines, "strip", lateral_count)
    second_bottom, second_raws = image_downward(arriving, jnp.maximum(vertical_slab - 1, 0))
    handed = jnp.where(vertical_slab == 0, above_floor_lines, second_bottom)
    first_section = (vertical_slab > 0).astype(jnp.float32)
    totals = [
        above_unscaled_waves[level] + first_section * second_raws[level] for level in range(LEVELS)
    ]
    selector = (jnp.arange(SECTIONS, dtype=jnp.int32) == vertical_slab).astype(jnp.float32)
    images = []
    for level in range(LEVELS):
        raw_image = totals[level]
        spread = lax.psum(selector * jnp.sum(raw_image * raw_image), "strip")
        mean_square = jnp.sum(spread * selector) / section_cells
        images.append(raw_image / jnp.sqrt(mean_square + 1e-06))
    return (jnp.stack(images, axis=0), handed)


SUB = 8
LANES = 128
PAD = 5
UNROLL = 8
TOGETHER = 4
MESH = pl.DeviceIdType.MESH


def at_row(row):
    return pl.ds(pl.multiple_of(row * SUB, SUB), SUB)


def kernel(
    strip_count,
    entry_ref,
    wave_ref,
    map_ref,
    table_ref,
    image_ref,
    handed_ref,
    starts,
    work,
    bottom,
    last,
    last_in,
    wave_out,
    map_out,
    map_all,
    raw,
    raw_in,
    sum_own,
    sum_in,
    swap_sems,
    halo_sems,
    hand_sems,
    fin_sems,
    raw_sems,
    sum_sems,
):
    nfh = wave_ref.shape[0] // 2
    length = wave_ref.shape[2]
    rows = 2 * length
    blocks = wave_ref.shape[3] // LANES
    lateral = strip_count // SECTIONS
    shift = lateral // 2
    pairs = lateral // 2
    margin = ORDER
    first = PAD + margin
    me = lax.axis_index("strip")
    position = lax.rem(me + strip_count - shift, strip_count)
    section = position // lateral
    place = lax.rem(position, lateral)
    pair = place // 2
    half = lax.rem(place, 2)
    up = jnp.where(pair > 0, 1, 0)
    down = jnp.where(pair < pairs - 1, 1, 0)
    has_up = pair > 0
    has_down = pair < pairs - 1
    has_before = section > 0
    has_after = section < SECTIONS - 1
    other = 1 - half

    def device(pos):
        return {"strip": lax.rem(pos + shift + strip_count, strip_count)}

    partner = device(position + 1 - 2 * half)
    upper = device(position - 2)
    lower = device(position + 2)
    deeper = device(position + lateral)
    shallower = device(position + strip_count - lateral)

    def remote(src, dst, sems, index, target):
        return pltpu.make_async_remote_copy(
            src_ref=src,
            dst_ref=dst,
            send_sem=sems.at[(0,) + index],
            recv_sem=sems.at[(1,) + index],
            device_id=target,
            device_id_type=MESH,
        )

    def span(row, count):
        return pl.ds(pl.multiple_of(row * SUB, SUB), count * SUB)

    zero = jnp.zeros((SUB, LANES), jnp.float32)
    for edge in (first - 1, first + rows):
        for f in range(nfh):
            for c in range(2):
                for s in range(2 * LEVELS):
                    starts[s, f, c, at_row(edge), :] = zero
        for c in range(2):
            for k in range(ORDER):
                work[k, c, at_row(edge), :] = zero

    barrier = pltpu.get_barrier_semaphore()
    for d in range(1, lateral):
        mate = device(section * lateral + lax.rem(place + d, lateral))
        pl.semaphore_signal(barrier, inc=1, device_id=mate, device_id_type=MESH)
    for target in (deeper, shallower):
        pl.semaphore_signal(barrier, inc=1, device_id=target, device_id_type=MESH)

    def rearrange(load, store):
        for g in range(length // SUB):
            for j in range(blocks):
                store(g, j, load(g, j))

    def strided(row, g, j):
        return pl.ds((row + g * SUB) * SUB + j, SUB, stride=SUB)

    own_row = half * length
    swaps = []
    for f in range(nfh):
        for c in range(2):
            rearrange(
                lambda g, j: wave_ref[other * nfh + f, c, pl.ds(g * SUB, SUB), pl.ds(j * LANES, LANES)],
                lambda g, j, x: pltpu_store(wave_out.at[f, c], strided(0, g, j), x),
            )
        if f == 0:
            pl.semaphore_wait(barrier, lateral + 1)
        copy = remote(
            wave_out.at[f],
            starts.at[0, f, :, span(first + own_row, length), :],
            swap_sems,
            (f,),
            partner,
        )
        copy.start()
        swaps.append(copy)
    for l in range(LEVELS):
        rearrange(
            lambda g, j: map_ref[l, pl.ds(g * SUB, SUB), pl.ds(j * LANES, LANES)],
            lambda g, j, x: pltpu_store(map_out.at[l], strided(0, g, j), x),
        )
    copy = remote(
        map_out, map_all.at[:, span(own_row, length), :], swap_sems, (nfh,), partner
    )
    copy.start()
    swaps.append(copy)
    for f in range(nfh):
        for c in range(2):
            rearrange(
                lambda g, j: wave_ref[half * nfh + f, c, pl.ds(g * SUB, SUB), pl.ds(j * LANES, LANES)],
                lambda g, j, x: pltpu_store(
                    starts.at[0, f, c], strided(first + own_row, g, j), x
                ),
            )
    for l in range(LEVELS):
        rearrange(
            lambda g, j: map_ref[l, pl.ds(g * SUB, SUB), pl.ds(j * LANES, LANES)],
            lambda g, j, x: pltpu_store(map_all.at[l], strided(own_row, g, j), x),
        )

    def halo_up(stage, f):
        ref = starts.at[stage, f]
        return remote(
            ref.at[:, span(first, margin), :],
            ref.at[:, span(first + rows, margin), :],
            halo_sems,
            (stage, f, 0),
            upper,
        )

    def halo_down(stage, f):
        ref = starts.at[stage, f]
        return remote(
            ref.at[:, span(first + rows - margin, margin), :],
            ref.at[:, span(first - margin, margin), :],
            halo_sems,
            (stage, f, 1),
            lower,
        )

    def send_halo(stage, f):
        pl.when(has_up)(lambda: halo_up(stage, f).start())
        pl.when(has_down)(lambda: halo_down(stage, f).start())

    def wait_halo(stage, f):
        pl.when(has_down)(lambda: halo_up(stage, f).wait_recv())
        pl.when(has_up)(lambda: halo_down(stage, f).wait_recv())

    def hand_parts(f):
        parts = ((0, margin), (rows - margin, margin), (margin, rows - 2 * margin))
        return [
            remote(
                bottom.at[f, :, span(row, count), :],
                starts.at[LEVELS, f, :, span(first + row, count), :],
                hand_sems,
                (f, n),
                deeper,
            )
            for n, (row, count) in enumerate(parts)
        ]

    lane = lax.broadcasted_iota(jnp.int32, (SUB, LANES), 1)
    sub = lax.broadcasted_iota(jnp.int32, (SUB, LANES), 0)
    at_first = lane == 0
    at_last = lane == LANES - 1
    keep_first = sub > 0
    keep_last = sub < SUB - 1

    def across(u):
        right = pltpu.roll(u, 1, 1)
        right_fix = jnp.where(keep_first, pltpu.roll(right, 1, 0), 0.0)
        left = pltpu.roll(u, LANES - 1, 1)
        left_fix = jnp.where(keep_last, pltpu.roll(left, SUB - 1, 0), 0.0)
        return jnp.where(at_first, right_fix, right) + jnp.where(at_last, left_fix, left)

    def reach(k):
        return ((margin - k + UNROLL - 1) // UNROLL) * UNROLL

    def apply(k, present, before, target):
        extra = reach(k)
        low = first - up * extra
        count = (rows + (up + down) * extra) // UNROLL

        def block(i, carry):
            base = low + i * UNROLL
            v = [
                [present[c, at_row(base - 1 + n), :] for n in range(UNROLL + 2)]
                for c in range(2)
            ]
            old = None
            if before is not None:
                old = [
                    [before[c, at_row(base + n), :] for n in range(UNROLL)] for c in range(2)
                ]
            values = []
            for c in range(2):
                q = [v[c][n] + v[c][n + 1] for n in range(UNROLL + 1)]
                for n in range(UNROLL):
                    u = q[n] + q[n + 1]
                    w = across(u) + (u + u)
                    centre = v[c][n + 1]
                    if old is None:
                        value = 0.125 * w - centre
                    else:
                        value = 0.25 * w - (centre + centre + old[c][n])
                    values.append(value)
            for c in range(2):
                for n in range(UNROLL):
                    target[c, at_row(base + n), :] = values[c * UNROLL + n]
            return carry

        lax.fori_loop(0, count, block, 0)

    def unit(tick, level, f, meanwhile=None):
        stage = tick * LEVELS + level
        start = starts.at[stage, f]
        apply(1, start, None, work.at[0])
        apply(2, work.at[0], start, work.at[1])

        def step(k, carry):
            apply(k, work.at[k - 2], work.at[k - 3], work.at[k - 1])
            return carry

        lax.fori_loop(3, ORDER + 1, step, 0)
        if meanwhile is not None:
            meanwhile()
        batch = section if tick == 0 else jnp.maximum(section - 1, 0)
        entry = entry_ref[batch, half * nfh + f]

        def combine(i, carry):
            spots = [TOGETHER * i + n for n in range(TOGETHER)]
            bins = [map_all[level, at_row(r), :] for r in spots]
            real = [None] * TOGETHER
            imag = [None] * TOGETHER
            for n, r in enumerate(spots):
                for k in range(ORDER + 1):
                    cr, ci = (
                        jnp.take_along_axis(
                            jnp.broadcast_to(
                                table_ref[entry, pl.ds(2 * k + c, 1), :], (SUB, LANES)
                            ),
                            bins[n],
                            axis=1,
                            mode="promise_in_bounds",
                        )
                        for c in range(2)
                    )
                    source = start if k == 0 else work.at[k - 1]
                    tr = source[0, at_row(first + r), :]
                    ti = source[1, at_row(first + r), :]
                    re = cr * tr - ci * ti
                    im = cr * ti + ci * tr
                    real[n] = re if k == 0 else real[n] + re
                    imag[n] = im if k == 0 else imag[n] + im
            for n, r in enumerate(spots):
                re, im = real[n], imag[n]
                if tick == 0 and f == 0:
                    raw[level, at_row(r), :] = re
                else:
                    part = re if tick == 0 else jnp.where(has_before, re, 0.0)
                    raw[level, at_row(r), :] = raw[level, at_row(r), :] + part
                for c, value in enumerate((re, im)):
                    if level < LEVELS - 1:
                        starts[stage + 1, f, c, at_row(first + r), :] = value
                    elif tick == 0:
                        bottom[f, c, at_row(r), :] = value
                    else:
                        last[f, c, at_row(r), :] = jnp.where(
                            has_before, value, bottom[f, c, at_row(r), :]
                        )
            return carry

        lax.fori_loop(0, rows // TOGETHER, combine, 0)

    def finish_wave(f):
        return remote(
            last.at[f, :, span(other * length, length), :],
            last_in.at[f],
            fin_sems,
            (f,),
            partner,
        )

    def finish_raw(l):
        return remote(
            raw.at[l, span(other * length, length), :], raw_in.at[l], raw_sems, (l,), partner
        )

    for f in range(nfh):
        swaps[f].wait_recv()
        send_halo(0, f)
    swaps[nfh].wait_recv()
    for level in range(LEVELS):
        for f in range(nfh):
            wait_halo(level, f)
            unit(0, level, f)
            if level < LEVELS - 1:
                send_halo(level + 1, f)
            else:

                @pl.when(has_after)
                def _():
                    for copy in hand_parts(f):
                        copy.start()

    def forward(f):
        @pl.when(has_before)
        def _():
            high, low, mid = hand_parts(f)
            high.wait_recv()
            pl.when(has_up)(lambda: halo_up(LEVELS, f).start())
            low.wait_recv()
            pl.when(has_down)(lambda: halo_down(LEVELS, f).start())
            mid.wait_recv()

    def skip_or(fn):
        pl.when(has_before)(fn)

    forward(0)
    for level in range(LEVELS):
        for f in range(nfh):

            @pl.when(has_before)
            def _():
                wait_halo(LEVELS + level, f)

            later = f + 1 if level == 0 and f + 1 < nfh else None
            unit(1, level, f, None if later is None else lambda: forward(later))
            if level < LEVELS - 1:

                @pl.when(has_before)
                def _():
                    send_halo(LEVELS + level + 1, f)

            else:
                finish_wave(f).start()
        finish_raw(level).start()

    for l in range(LEVELS):
        finish_raw(l).wait_recv()

        def merge(i, carry):
            value = raw[l, at_row(own_row + i), :] + raw_in[l, at_row(i), :]
            raw_in[l, at_row(i), :] = value
            return carry + value * value

        sum_own[pl.ds(l * SUB, SUB), :] = lax.fori_loop(0, length, merge, zero)
    for d in range(1, lateral):
        mate = device(section * lateral + lax.rem(place + d, lateral))
        remote(sum_own, sum_in.at[d], sum_sems, (d,), mate).start()

    for f in range(nfh):
        for c in range(2):
            rearrange(
                lambda g, j: last[f, c, strided(own_row, g, j), :],
                lambda g, j, x: out_store(handed_ref, half * nfh + f, c, g, j, x),
            )
    for f in range(nfh):
        finish_wave(f).wait_recv()
        for c in range(2):
            rearrange(
                lambda g, j: last_in[f, c, strided(0, g, j), :],
                lambda g, j, x: out_store(handed_ref, other * nfh + f, c, g, j, x),
            )

    total = sum_own[...]
    for d in range(1, lateral):
        mate = device(section * lateral + lax.rem(place + d, lateral))
        remote(sum_own, sum_in.at[d], sum_sems, (d,), mate).wait_recv()
        total = total + sum_in[d]
    cells = length * lateral * blocks * LANES
    for l in range(LEVELS):
        mean = jnp.sum(total[l * SUB : (l + 1) * SUB], axis=(0, 1), keepdims=True) / cells
        scale = jnp.broadcast_to(1.0 / jnp.sqrt(mean + 1e-06), (SUB, LANES))

        def put(g, j, x):
            image_ref[l, pl.ds(g * SUB, SUB), pl.ds(j * LANES, LANES)] = x * scale

        rearrange(lambda g, j: raw_in[l, strided(0, g, j), :], put)

    for copy in swaps:
        copy.wait_send()
    for f in range(nfh):
        send_done = lambda make, stage: make(stage, f).wait_send()
        for stage in range(2 * LEVELS):
            live_up = has_up if stage < LEVELS else has_up & has_before
            live_down = has_down if stage < LEVELS else has_down & has_before
            pl.when(live_up)(lambda: send_done(halo_up, stage))
            pl.when(live_down)(lambda: send_done(halo_down, stage))

        @pl.when(has_after)
        def _():
            for copy in hand_parts(f):
                copy.wait_send()

        finish_wave(f).wait_send()
    for l in range(LEVELS):
        finish_raw(l).wait_send()
    for d in range(1, lateral):
        mate = device(section * lateral + lax.rem(place + d, lateral))
        remote(sum_own, sum_in.at[d], sum_sems, (d,), mate).wait_send()


def pltpu_store(ref, where, x):
    ref[where, :] = x


def out_store(ref, f, c, g, j, x):
    ref[f, c, pl.ds(g * SUB, SUB), pl.ds(j * LANES, LANES)] = x


def paired(
    incoming_wave,
    speed_class_map,
    spectral_entry_index,
    filter_weights,
    scaled_pulsations,
    inverse_speed_classes,
):
    strip_count = lax.axis_size("strip")
    lateral = strip_count // SECTIONS
    length = incoming_wave.shape[2]
    nfh = NFREQ // 2
    rows = 2 * length
    tall = (rows + 2 * ORDER + 2 * PAD) * SUB
    angle = scaled_pulsations[:, None] * inverse_speed_classes[None, :]
    cosine = jnp.cos(angle)[:, None, :]
    sine = jnp.sin(angle)[:, None, :]
    by_order = jnp.transpose(filter_weights, (2, 0, 3, 1))
    real = by_order[0] * cosine - by_order[1] * sine
    imag = by_order[0] * sine + by_order[1] * cosine
    table = jnp.stack([real, imag], axis=2).reshape(NW, 2 * (ORDER + 1), NBIN)
    table = jnp.pad(table, ((0, 0), (0, 0), (0, LANES - NBIN)))
    f32 = jnp.float32
    vmem = pl.BlockSpec(memory_space=pltpu.VMEM)

    def dma(*shape):
        return pltpu.SemaphoreType.DMA((2,) + shape)

    return pl.pallas_call(
        functools.partial(kernel, strip_count),
        out_shape=(
            jax.ShapeDtypeStruct(speed_class_map.shape, f32),
            jax.ShapeDtypeStruct(incoming_wave.shape, f32),
        ),
        in_specs=[pl.BlockSpec(memory_space=pltpu.SMEM), vmem, vmem, vmem],
        out_specs=(vmem, vmem),
        scratch_shapes=[
            pltpu.VMEM((2 * LEVELS, nfh, 2, tall, LANES), f32),
            pltpu.VMEM((ORDER, 2, tall, LANES), f32),
            pltpu.VMEM((nfh, 2, rows * SUB, LANES), f32),
            pltpu.VMEM((nfh, 2, rows * SUB, LANES), f32),
            pltpu.VMEM((nfh, 2, length * SUB, LANES), f32),
            pltpu.VMEM((nfh, 2, length * SUB, LANES), f32),
            pltpu.VMEM((LEVELS, length * SUB, LANES), jnp.int32),
            pltpu.VMEM((LEVELS, rows * SUB, LANES), jnp.int32),
            pltpu.VMEM((LEVELS, rows * SUB, LANES), f32),
            pltpu.VMEM((LEVELS, length * SUB, LANES), f32),
            pltpu.VMEM((LEVELS * SUB, LANES), f32),
            pltpu.VMEM((lateral, LEVELS * SUB, LANES), f32),
            dma(nfh + 1),
            dma(2 * LEVELS, nfh, 2),
            dma(nfh, 3),
            dma(nfh),
            dma(LEVELS),
            dma(lateral),
        ],
        compiler_params=pltpu.CompilerParams(
            collective_id=0, has_side_effects=True, vmem_limit_bytes=48 * 1024 * 1024
        ),
    )(spectral_entry_index, incoming_wave, speed_class_map, table)


def fits(mesh):
    lateral = mesh.shape["strip"] // SECTIONS
    return NFREQ % 2 == 0 and lateral % 4 == 0


def body_for(mesh):
    def body(wave, *rest):
        whole = wave.shape[3] == SUB * LANES and wave.shape[2] % SUB == 0
        if fits(mesh) and whole and wave.shape[2] >= ORDER:
            return paired(wave, *rest)
        return shards(wave, *rest)

    return body


def solution(mesh):
    return jax.shard_map(
        body_for(mesh),
        mesh=mesh,
        in_specs=(
            P("groups", None, "strip", None),
            P("groups", "strip", None),
            P("groups", None),
            P(),
            P(),
            P(),
        ),
        out_specs=(P("groups", "strip", None), P("groups", None, "strip", None)),
        check_vma=False,
    )
```
